32 devices in a mesh: site: 2 (over y), pts: 16 (over z, x, core).
Axes of the slice: x: 2, y: 2, z: 4, core: 2. Of those that a mesh axis runs over, the one named last changes fastest.
Arguments:
- green_tensors: bfloat16 [512, 4, 6, 2, 1024], P(('site', 'pts')), parts along dimension 0, may hold values from -6 to 6
- block_lists: int32 [32, 32], P(('site', 'pts')), parts along dimension 0, may hold values from 0 to 255, as said below
- block_count: int32 [32], P(('site', 'pts')), parts along dimension 0, may hold values from 1 to 32
- onset_steps: int32 [32, 16, 128], P(('site', 'pts')), parts along dimension 0, may hold values from 0 to 255
- slip_amount: float32 [32, 16, 128], P(('site', 'pts')), parts along dimension 0, may hold values from 0.2 to 2
- mechanism: float32 [32, 6], P(('site', 'pts')), parts along dimension 0, may hold values from -2.4 to 2.4
- slip_rate: float32 [32, 16, 128], P(('site', 'pts')), parts along dimension 0, may hold values from 0.005 to 0.05
Outputs:
- seismograms: float32 [32, 16, 2, 1024], P(('site', 'pts')), parts along dimension 0
The draws below stay inside these ranges and needn't reach their ends.
There are 2 independent parts, one for each index of `site`. The reference program is written for one: setup_inputs(seed, part) draws one part's arguments, and reference() takes and returns one part's arrays. A program takes and returns all parts, laid end to end along the dimension named above; each array names one. Nothing has to cross between parts.
Inputs may be any that keep to these rules, and one draw needn't show every extreme that they name: `block_lists`: numbers of point blocks; the ruptures held by one device name at most 2 entries in blocks held by any one device, and exactly 2 for some holder.
All inputs are finite; a program needn't handle non-finite values.
Results may differ from the reference program's by a relative error of at most 0.0003.
Values may be sent and summed in bfloat16 or wider, within the bound.
A program may use at most 128 MiB of HBM per device.

```python
import math
import jax
import jax.numpy as jnp
from jax import lax

NT = 1024
P_SIZE = 4
K = 32
V = 16
L = 128
MAXON = 256
BD = 16
RD = 1
NB = 256
R = 16
N_PTS = 16


def draw_block_lists(key, part):
    entries = RD * K

    def per_worker(worker):
        worker_key = jax.random.fold_in(jax.random.fold_in(key, 11), worker)
        holders = jax.random.permutation(worker_key, N_PTS)
        order = jnp.arange(entries, dtype=jnp.int32)
        holder_of = holders[order % N_PTS]
        local_block = jax.random.randint(jax.random.fold_in(worker_key, 1), (entries,), 0, BD)
        return (holder_of * BD + local_block).astype(jnp.int32)
    lists = jax.vmap(per_worker)(jnp.arange(N_PTS, dtype=jnp.int32))
    return lists.reshape(RD * N_PTS, K)


def set_ends(values, own_key, low, top_value):
    index_at = [jax.random.randint(jax.random.fold_in(own_key, axis), (), 0, length) for axis, length in enumerate(values.shape)]
    main_axis = values.shape.index(max(values.shape))
    beside = index_at[:main_axis] + [(index_at[main_axis] + 1) % values.shape[main_axis]] + index_at[main_axis + 1:]
    return values.at[tuple(index_at)].set(low).at[tuple(beside)].set(top_value)


def steps_of(own_key, dims, cuts, smallest, top_value):
    def one(dim, blocks):
        draws = jax.random.uniform(jax.random.fold_in(jax.random.fold_in(own_key, 6), dim), (blocks,), jnp.float32, smallest / len(cuts), top_value / len(cuts))
        return jnp.repeat(jnp.exp(draws), dims[dim] // blocks).reshape((-1,) + (1,) * (len(dims) - dim - 1))

    gain = one(*cuts[0])
    for cut in cuts[1:]:
        gain = gain * one(*cut)
    return gain


def normal_values(rng, shape, scale, limit, cuts=(), kind=jnp.bfloat16):
    array = scale * jax.random.normal(rng, shape, jnp.float32)
    if cuts:
        array = array * steps_of(rng, shape, cuts, -0.22, 0.18)
    return jnp.clip(array, -limit, limit).astype(kind)


def setup_inputs(seed: int = 0, part: int = 0) -> dict:
    keys = jax.random.split(jax.random.key(seed), 8)
    part_keys = jax.random.split(jax.random.fold_in(keys[7], part), 8)
    return {
        "green_tensors": normal_values(part_keys[0], (NB, P_SIZE, 6, 2, NT), 1.0, 6.0, ((0, 16),)),
        "block_lists": draw_block_lists(jax.random.fold_in(jax.random.fold_in(keys[7], part), 71), part),
        "block_count": set_ends(jax.random.randint(part_keys[2], (R,), 1, K + 1), jax.random.fold_in(part_keys[2], 1), 1, K).astype(jnp.int32),
        "onset_steps": set_ends(jax.random.randint(part_keys[3], (R, V, K * P_SIZE), 0, MAXON), jax.random.fold_in(part_keys[3], 1), 0, MAXON - 1).astype(jnp.int32),
        "slip_amount": jnp.clip(jnp.exp(math.log(2.0) - 2.3025851 * jax.random.uniform(part_keys[4], (R, V, K * P_SIZE), jnp.float32) ** steps_of(part_keys[4], (R, V, K * P_SIZE), ((0, 16),), -0.2, 0.2)), 0.2, 2.0),
        "mechanism": normal_values(part_keys[5], (R, 6), 0.4, 2.4, ((0, 16),), jnp.float32),
        "slip_rate": jnp.clip(jnp.exp(math.log(0.05) - 2.3025851 * jax.random.uniform(part_keys[6], (R, V, L), jnp.float32) ** steps_of(part_keys[6], (R, V, L), ((0, 16),), -0.2, 0.2)), 0.005, 0.05),
    }


def lag_traces(traces, onsets):
    steps = jnp.arange(traces.shape[-1], dtype=jnp.int32)
    source = steps[None, :] - onsets[:, None]
    inside = source >= 0
    picked = jnp.take_along_axis(traces, jnp.broadcast_to(jnp.maximum(source, 0)[:, None, :], traces.shape), axis=2)
    return jnp.where(inside[:, None, :], picked, 0.0)


def weighted_sum(traces, weights, onsets):
    def per_variation(weight_row, onset_row):
        return jnp.sum(weight_row[:, None, None] * lag_traces(traces, onset_row), axis=0)
    return jax.vmap(per_variation)(weights, onsets)


def reference(green_tensors, block_lists, block_count, onset_steps, slip_amount, mechanism, slip_rate):
    listed = block_lists.shape[1]
    length = green_tensors.shape[-1]

    def per_rupture(inputs):
        blocks, listed_count, onset_rows, slip_rows, mech_row, rate_rows = inputs
        chosen = jnp.take(green_tensors, blocks, axis=0).astype(jnp.float32)
        traces = jnp.einsum("kpsct,s->kpct", chosen, mech_row, precision=lax.Precision.HIGHEST)
        kept_mask = (jnp.arange(listed, dtype=jnp.int32) < listed_count).astype(jnp.float32)
        points = chosen.shape[1]
        weights = slip_rows * jnp.repeat(kept_mask, points)[None, :]
        motion = weighted_sum(traces.reshape(-1, 2, length), weights, onset_rows)

        def convolve_row(signal, kernel):
            return jnp.convolve(signal, kernel, precision=lax.Precision.HIGHEST)[:length]

        return jax.vmap(jax.vmap(convolve_row, (0, None)), (0, 0))(motion, rate_rows)

    return lax.map(per_rupture, (block_lists, block_count, onset_steps, slip_amount, mechanism, slip_rate))
```

```python
import functools

import jax
import jax.numpy as jnp
from jax import lax
from jax.experimental import pallas as pl
from jax.experimental.pallas import tpu as pltpu
from jax.sharding import PartitionSpec as P

LANES = 128


def exchange_kernel(n, cap, width, wants_ref, mech_ref, green_ref, out_ref,
                    wanted, mechs, wanted_s, outbox, send_w, recv_w, send_m, recv_m,
                    local_sem, send_t, recv_t):
    me = lax.axis_index("pts")

    barrier = pltpu.get_barrier_semaphore()

    def greet(d, carry):
        pl.semaphore_signal(barrier, inc=1, device_id={"pts": lax.rem(me + d, n)},
                            device_id_type=pl.DeviceIdType.MESH)
        return carry

    lax.fori_loop(1, n, greet, 0)
    pl.semaphore_wait(barrier, n - 1)

    def want_copy(d):
        peer = lax.rem(me + d, n)
        return pltpu.make_async_remote_copy(
            src_ref=wants_ref.at[peer], dst_ref=wanted.at[n - d],
            send_sem=send_w.at[d], recv_sem=recv_w.at[n - d],
            device_id={"pts": peer}, device_id_type=pl.DeviceIdType.MESH)

    def mech_copy(d):
        peer = lax.rem(me + d, n)
        return pltpu.make_async_remote_copy(
            src_ref=mech_ref, dst_ref=mechs.at[n - d],
            send_sem=send_m.at[d], recv_sem=recv_m.at[n - d],
            device_id={"pts": peer}, device_id_type=pl.DeviceIdType.MESH)

    def start_meta(d, carry):
        want_copy(d).start()
        mech_copy(d).start()
        return carry

    lax.fori_loop(1, n, start_meta, 0)
    wanted[0] = wants_ref[me]
    mechs[0] = mech_ref[...]

    def wait_meta(d, carry):
        want_copy(d).wait()
        mech_copy(d).wait()
        return carry

    lax.fori_loop(1, n, wait_meta, 0)
    to_scalar = pltpu.make_async_copy(wanted, wanted_s, local_sem)
    to_scalar.start()
    to_scalar.wait()

    def traces_for(d, slot):
        lhs = mechs[d][:, :width]
        high = lhs.astype(jnp.bfloat16).astype(jnp.float32)
        rest = lhs - high
        mid = rest.astype(jnp.bfloat16).astype(jnp.float32)
        stack = jnp.concatenate([high, mid, rest - mid], axis=0).astype(jnp.bfloat16)
        block = green_ref[wanted_s[d, 0, slot]]
        parts = jnp.dot(stack, block, preferred_element_type=jnp.float32)
        m = lhs.shape[0]
        return parts[0:m] + (parts[m:2 * m] + parts[2 * m:3 * m])

    def trace_copy(d):
        peer = lax.rem(me + d, n)
        return pltpu.make_async_remote_copy(
            src_ref=outbox.at[d], dst_ref=out_ref.at[me],
            send_sem=send_t.at[d], recv_sem=recv_t.at[n - d],
            device_id={"pts": peer}, device_id_type=pl.DeviceIdType.MESH)

    def step(d, carry):
        for slot in range(cap):
            outbox[d, slot] = traces_for(d, slot)

        @pl.when(d > 1)
        def _():
            trace_copy(d - 1).start()

        return carry

    lax.fori_loop(1, n, step, 0)
    for slot in range(cap):
        out_ref[me, slot] = traces_for(0, slot)
    trace_copy(n - 1).start()

    def wait_traces(d, carry):
        trace_copy(d).wait()
        return carry

    lax.fori_loop(1, n, wait_traces, 0)


def motion_kernel(points, comps, rows_ref, count_ref, traces_ref, onset_ref, slip_ref, rate_ref,
                  out_ref, motion):
    variations = onset_ref.shape[0]
    length = traces_ref.shape[-1]
    tiles = length // LANES
    lane = lax.broadcasted_iota(jnp.int32, (8, LANES), 1)
    motion[0:comps] = jnp.zeros((comps,) + motion.shape[1:], jnp.float32)
    for group in range(variations // 8):
        onsets = onset_ref[group * 8:group * 8 + 8, :]
        slips = slip_ref[group * 8:group * 8 + 8, :]

        def body(k, acc):
            acc = list(acc)
            row = rows_ref[k]
            for p in range(points):
                pick = jnp.full((8, LANES), k * points + p, jnp.int32)
                onset = jnp.take_along_axis(onsets, pick, axis=1)
                slip = jnp.take_along_axis(slips, pick, axis=1)
                shift = jnp.bitwise_and(onset, LANES - 1)
                back = jnp.right_shift(onset, 7) + (lane >= LANES - shift).astype(jnp.int32)
                one = back >= 1
                two = back >= 2
                source = jnp.bitwise_and(lane - shift, LANES - 1)
                for c in range(comps):
                    prev2 = jnp.zeros((8, LANES), jnp.float32)
                    prev1 = prev2
                    for i in range(tiles):
                        cur = jnp.broadcast_to(
                            traces_ref[row, pl.ds(p * comps + c, 1), i * LANES:(i + 1) * LANES],
                            (8, LANES))
                        mixed = jnp.where(two, prev2, jnp.where(one, prev1, cur))
                        acc[i * comps + c] += slip * jnp.take_along_axis(mixed, source, axis=1)
                        prev2, prev1 = prev1, cur
            return tuple(acc)

        zero = jnp.zeros((8, LANES), jnp.float32)
        acc = lax.fori_loop(0, count_ref[0], body, (zero,) * (tiles * comps))
        for j in range(tiles * comps):
            motion[comps + j, group * 8:group * 8 + 8, :] = acc[j]

    count = tiles * comps
    i_row = lax.broadcasted_iota(jnp.int32, (LANES, LANES), 0)
    j_lane = lax.broadcasted_iota(jnp.int32, (LANES, LANES), 1)
    near_mask = j_lane >= i_row
    for v in range(variations):
        rate = jnp.broadcast_to(rate_ref[v:v + 1, :], (LANES, LANES))
        turned = pltpu.roll(rate, 0, 1, stride=1, stride_axis=0)
        both = jnp.concatenate(
            [jnp.where(near_mask, turned, 0.0), jnp.where(near_mask, 0.0, turned)], axis=0)
        here = motion[comps:comps + count, v, :]
        before = motion[0:count, v, :]
        lhs = jnp.concatenate([here, before], axis=1)
        result = jnp.dot(lhs, both, precision=lax.Precision.HIGHEST,
                         preferred_element_type=jnp.float32)
        for i in range(tiles):
            out_ref[v, :, i * LANES:(i + 1) * LANES] = result[i * comps:(i + 1) * comps, :]


def local(green_tensors, block_lists, block_count, onset_steps, slip_amount, mechanism, slip_rate):
    held, points, strains, comps, length = green_tensors.shape
    ruptures, listed = block_lists.shape
    assert ruptures == 1
    variations = onset_steps.shape[1]
    n = lax.axis_size("pts")
    cap = max(1, listed // n)
    width = points * strains * comps
    rows_per = points * comps

    blocks = block_lists.reshape(listed)
    holder = blocks // held
    local_block = blocks % held
    order = jnp.arange(listed, dtype=jnp.int32)
    rank = jnp.sum(((holder[:, None] == holder[None, :]) & (order[None, :] < order[:, None]))
                   .astype(jnp.int32), axis=1)
    place = holder * cap + rank
    lanes = jnp.arange(LANES, dtype=jnp.int32)
    hit = (holder[None, None, :] == jnp.arange(n, dtype=jnp.int32)[:, None, None]) & (
        rank[None, None, :] == lanes[None, :, None])
    wants = jnp.sum(jnp.where(hit, local_block[None, None, :], 0), axis=2).reshape(n, 1, LANES)

    out_row = jnp.arange(rows_per, dtype=jnp.int32)[:, None]
    in_row = jnp.arange(LANES, dtype=jnp.int32)[None, :]
    same = (in_row // (strains * comps) == out_row // comps) & (in_row % comps == out_row % comps)
    strain_of = (in_row // comps) % strains
    mech = jnp.zeros((rows_per, LANES), jnp.float32)
    for s in range(strains):
        mech = jnp.where(same & (strain_of == s), mechanism[0, s], mech)

    vmem = pl.BlockSpec(memory_space=pltpu.VMEM)
    smem = pl.BlockSpec(memory_space=pltpu.SMEM)
    traces = pl.pallas_call(
        functools.partial(exchange_kernel, n, cap, width),
        out_shape=jax.ShapeDtypeStruct((n, cap, rows_per, length), jnp.float32),
        in_specs=[vmem, vmem, vmem],
        out_specs=vmem,
        scratch_shapes=[
            pltpu.VMEM((n, 1, LANES), jnp.int32),
            pltpu.VMEM((n, rows_per, LANES), jnp.float32),
            pltpu.SMEM((n, 1, LANES), jnp.int32),
            pltpu.VMEM((n, cap, rows_per, length), jnp.float32),
            pltpu.SemaphoreType.DMA((n,)),
            pltpu.SemaphoreType.DMA((n,)),
            pltpu.SemaphoreType.DMA((n,)),
            pltpu.SemaphoreType.DMA((n,)),
            pltpu.SemaphoreType.DMA,
            pltpu.SemaphoreType.DMA((n,)),
            pltpu.SemaphoreType.DMA((n,)),
        ],
        compiler_params=pltpu.CompilerParams(
            collective_id=0, has_side_effects=True, vmem_limit_bytes=48 << 20),
        name="exchange",
    )(wants, mech, green_tensors.reshape(held, width, length))

    seismograms = pl.pallas_call(
        functools.partial(motion_kernel, points, comps),
        out_shape=jax.ShapeDtypeStruct((variations, comps, length), jnp.float32),
        in_specs=[smem, smem, vmem, vmem, vmem, vmem],
        out_specs=vmem,
        scratch_shapes=[pltpu.VMEM(((length // LANES + 1) * comps, variations, LANES), jnp.float32)],
        compiler_params=pltpu.CompilerParams(vmem_limit_bytes=48 << 20),
        name="motion",
    )(place, block_count, traces.reshape(n * cap, rows_per, length),
      onset_steps[0], slip_amount[0], slip_rate[0])
    return seismograms[None]


def solution(mesh):
    in_specs = (
        P(("site", "pts"), None, None, None, None),
        P(("site", "pts"), None),
        P(("site", "pts")),
        P(("site", "pts"), None, None),
        P(("site", "pts"), None, None),
        P(("site", "pts"), None),
        P(("site", "pts"), None, None),
    )
    out_specs = P(("site", "pts"), None, None, None)
    return jax.shard_map(local, mesh=mesh, in_specs=in_specs, out_specs=out_specs, check_vma=False)
```

```python
import functools

import jax
import jax.numpy as jnp
from jax import lax
from jax.experimental import pallas as pl
from jax.experimental.pallas import tpu as pltpu
from jax.sharding import PartitionSpec as P

LANES = 128


def seismogram_kernel(n, cap, points, comps, width, listed, wants_s_ref, mech_s_ref, count_ref,
                      wants_ref, green_ref, onset_ref, slip_ref, rate_ref, out_ref,
                      wanted, mech, mechs, wanted_s, outbox, out_scale, inbox, in_scale, traces,
                      motion, high_taps, low_taps,
                      send_w, recv_w, send_m, recv_m, local_sem, send_t, recv_t, send_s, recv_s):
    me = lax.axis_index("pts")
    rows = points * comps
    length = traces.shape[-1]
    tiles = length // LANES
    half = tiles // 2
    strains = width // rows
    variations = onset_ref.shape[0]
    mesh_id = pl.DeviceIdType.MESH
    lane = lax.broadcasted_iota(jnp.int32, (8, LANES), 1)
    sub = lax.broadcasted_iota(jnp.int32, (8, LANES), 0)

    barrier = pltpu.get_barrier_semaphore()

    def greet(d, carry):
        pl.semaphore_signal(barrier, inc=1, device_id={"pts": lax.rem(me + d, n)},
                            device_id_type=mesh_id)
        return carry

    lax.fori_loop(1, n, greet, 0)

    out_row = lax.broadcasted_iota(jnp.int32, (rows, LANES), 0)
    in_row = lax.broadcasted_iota(jnp.int32, (rows, LANES), 1)
    table = jnp.zeros((rows, LANES), jnp.float32)
    for p in range(points):
        for s in range(strains):
            for c in range(comps):
                here = (out_row == p * comps + c) & (in_row == (p * strains + s) * comps + c)
                table = jnp.where(here, mech_s_ref[0, s], table)
    mech[...] = table
    mechs[0] = table
    wanted[0] = wants_ref[me]
    pl.semaphore_wait(barrier, n - 1)

    def remote(src, dst, send, recv, d):
        return pltpu.make_async_remote_copy(
            src_ref=src, dst_ref=dst.at[n - d], send_sem=send.at[d], recv_sem=recv.at[n - d],
            device_id={"pts": lax.rem(me + d, n)}, device_id_type=mesh_id)

    def want_copy(d):
        return remote(wants_ref.at[lax.rem(me + d, n)], wanted, send_w, recv_w, d)

    def mech_copy(d):
        return remote(mech, mechs, send_m, recv_m, d)

    def trace_copy(d):
        return remote(outbox.at[d], inbox, send_t, recv_t, d)

    def scale_copy(d):
        return remote(out_scale.at[d], in_scale, send_s, recv_s, d)

    def start_meta(d, carry):
        want_copy(d).start()
        mech_copy(d).start()
        return carry

    lax.fori_loop(1, n, start_meta, 0)

    def wait_meta(d, carry):
        want_copy(d).wait()
        mech_copy(d).wait()
        return carry

    lax.fori_loop(1, n, wait_meta, 0)
    to_scalar = pltpu.make_async_copy(wanted, wanted_s, local_sem)
    to_scalar.start()
    to_scalar.wait()

    def encode(d, box, scale_box, at):
        lhs = mechs[d][:, :width]
        high = lhs.astype(jnp.bfloat16).astype(jnp.float32)
        rest = lhs - high
        mid = rest.astype(jnp.bfloat16).astype(jnp.float32)
        stack = jnp.concatenate([high, mid, rest - mid], axis=0).astype(jnp.bfloat16)
        scales = jnp.zeros((8, LANES), jnp.float32)
        for slot in range(cap):
            block = green_ref[wanted_s[d, 0, slot]]
            parts = jnp.dot(stack, block, preferred_element_type=jnp.float32)
            full = parts[0:rows] + (parts[rows:2 * rows] + parts[2 * rows:3 * rows])
            coded = []
            for i in range(tiles):
                part = full[:, i * LANES:(i + 1) * LANES]
                top = jnp.max(jnp.abs(part), axis=1, keepdims=True)
                inverse = 32767.0 / jnp.maximum(top, 1e-30)
                coded.append(jnp.floor(part * inverse + 0.5).astype(jnp.int32))
                scales = jnp.where(lane == (slot * tiles + i) * rows + sub,
                                   top * (1.0 / 32767.0), scales)
            for i in range(half):
                word = jnp.bitwise_or(jnp.left_shift(coded[i + half], 16),
                                      jnp.bitwise_and(coded[i], 0xFFFF))
                box[at, slot, :, i * LANES:(i + 1) * LANES] = word
        scale_box[at] = jnp.sum(scales, axis=0, keepdims=True)

    def send(d, carry):
        encode(d, outbox, out_scale, d)

        @pl.when(d > 1)
        def _():
            trace_copy(d - 1).start()
            scale_copy(d - 1).start()

        return carry

    lax.fori_loop(1, n, send, 0)
    encode(0, inbox, in_scale, 0)
    trace_copy(n - 1).start()
    scale_copy(n - 1).start()

    i_row = lax.broadcasted_iota(jnp.int32, (LANES, LANES), 0)
    j_lane = lax.broadcasted_iota(jnp.int32, (LANES, LANES), 1)
    near_mask = j_lane >= i_row
    motion[...] = jnp.zeros(motion.shape, jnp.float32)

    for v in range(variations):
        rate = jnp.broadcast_to(rate_ref[v:v + 1, :], (LANES, LANES))
        turned = pltpu.roll(rate, 0, 1, stride=1, stride_axis=0)
        both = jnp.concatenate(
            [jnp.where(near_mask, turned, 0.0), jnp.where(near_mask, 0.0, turned)], axis=0)
        high = both.astype(jnp.bfloat16)
        high_taps[v] = high
        low_taps[v] = (both - high.astype(jnp.float32)).astype(jnp.bfloat16)

    def arrive(step, carry):
        j = lax.rem(n - step, n)
        source_device = lax.rem(me + j, n)

        @pl.when(step > 0)
        def _():
            trace_copy(step).wait_recv()
            scale_copy(step).wait_recv()

        scales = jnp.broadcast_to(in_scale[j], (8, LANES))
        for slot in range(cap):
            for i in range(half):
                word = inbox[j, slot, :, i * LANES:(i + 1) * LANES]
                low = jnp.right_shift(jnp.left_shift(word, 16), 16)
                high = jnp.right_shift(word, 16)
                for at, value in ((i, low), (i + half, high)):
                    scale = jnp.take_along_axis(scales, (slot * tiles + at) * rows + sub, axis=1)
                    traces[slot, :, at * LANES:(at + 1) * LANES] = (
                        value.astype(jnp.float32) * scale)
        for group in range(variations // 8):
            onsets = onset_ref[group * 8:group * 8 + 8, :]
            slips = slip_ref[group * 8:group * 8 + 8, :]
            acc = [motion[comps + q, group * 8:group * 8 + 8, :] for q in range(tiles * comps)]
            for slot in range(cap):
                k = wants_s_ref[source_device, 0, cap + slot]
                used = jnp.where(jnp.full((8, LANES), k, jnp.int32) < count_ref[0], 1.0, 0.0)
                base = jnp.minimum(jnp.full((8, LANES), k, jnp.int32), listed - 1) * points
                for p in range(points):
                    onset = jnp.take_along_axis(onsets, base + p, axis=1)
                    slip = jnp.take_along_axis(slips, base + p, axis=1) * used
                    shift = jnp.bitwise_and(onset, LANES - 1)
                    back = jnp.right_shift(onset, 7) + (lane >= LANES - shift).astype(jnp.int32)
                    one = back >= 1
                    two = back >= 2
                    source = jnp.bitwise_and(lane - shift, LANES - 1)
                    for c in range(comps):
                        prev2 = jnp.zeros((8, LANES), jnp.float32)
                        prev1 = prev2
                        for i in range(tiles):
                            cur = jnp.broadcast_to(
                                traces[slot, p * comps + c:p * comps + c + 1,
                                       i * LANES:(i + 1) * LANES], (8, LANES))
                            mixed = jnp.where(two, prev2, jnp.where(one, prev1, cur))
                            acc[i * comps + c] += slip * jnp.take_along_axis(mixed, source, axis=1)
                            prev2, prev1 = prev1, cur
            for q in range(tiles * comps):
                motion[comps + q, group * 8:group * 8 + 8, :] = acc[q]
        return carry

    lax.fori_loop(0, n, arrive, 0)

    count = tiles * comps
    for v in range(variations):
        lhs = jnp.concatenate([motion[comps:comps + count, v, :], motion[0:count, v, :]], axis=1)
        high = lhs.astype(jnp.bfloat16).astype(jnp.float32)
        pair = jnp.concatenate([high, lhs - high], axis=0).astype(jnp.bfloat16)
        main = jnp.dot(pair, high_taps[v], preferred_element_type=jnp.float32)
        minor = jnp.dot(pair[:count], low_taps[v], preferred_element_type=jnp.float32)
        result = main[:count] + (main[count:] + minor)
        for i in range(tiles):
            out_ref[v, :, i * LANES:(i + 1) * LANES] = result[i * comps:(i + 1) * comps, :]

    def wait_sent(d, carry):
        trace_copy(d).wait_send()
        scale_copy(d).wait_send()
        return carry

    lax.fori_loop(1, n, wait_sent, 0)


def local(green_tensors, block_lists, block_count, onset_steps, slip_amount, mechanism, slip_rate):
    held, points, strains, comps, length = green_tensors.shape
    ruptures, listed = block_lists.shape
    assert ruptures == 1
    variations = onset_steps.shape[1]
    n = lax.axis_size("pts")
    cap = max(1, listed // n)
    width = points * strains * comps
    rows = points * comps
    tiles = length // LANES
    assert cap * tiles * rows <= LANES

    blocks = block_lists.reshape(listed)
    holder = blocks // held
    order = jnp.arange(listed, dtype=jnp.int32)
    rank = jnp.sum(((holder[:, None] == holder[None, :]) & (order[None, :] < order[:, None]))
                   .astype(jnp.int32), axis=1)
    lanes = jnp.arange(LANES, dtype=jnp.int32)
    hit = (holder[None, None, :] == jnp.arange(n, dtype=jnp.int32)[:, None, None]) & (
        rank[None, None, :] == (lanes % cap)[None, :, None])
    value = jnp.where((lanes < cap)[None, :, None], (blocks % held)[None, None, :],
                      (order - listed)[None, None, :])
    wants = jnp.sum(jnp.where(hit, value, 0), axis=2) + jnp.where(lanes < cap, 0, listed)[None, :]
    wants = wants.astype(jnp.int32).reshape(n, 1, LANES)

    vmem = pl.BlockSpec(memory_space=pltpu.VMEM)
    smem = pl.BlockSpec(memory_space=pltpu.SMEM)
    dma = pltpu.SemaphoreType.DMA
    seismograms = pl.pallas_call(
        functools.partial(seismogram_kernel, n, cap, points, comps, width, listed),
        out_shape=jax.ShapeDtypeStruct((variations, comps, length), jnp.float32),
        in_specs=[smem, smem, smem, vmem, vmem, vmem, vmem, vmem],
        out_specs=vmem,
        scratch_shapes=[
            pltpu.VMEM((n, 1, LANES), jnp.int32),
            pltpu.VMEM((rows, LANES), jnp.float32),
            pltpu.VMEM((n, rows, LANES), jnp.float32),
            pltpu.SMEM((n, 1, LANES), jnp.int32),
            pltpu.VMEM((n, cap, rows, length // 2), jnp.int32),
            pltpu.VMEM((n, 1, LANES), jnp.float32),
            pltpu.VMEM((n, cap, rows, length // 2), jnp.int32),
            pltpu.VMEM((n, 1, LANES), jnp.float32),
            pltpu.VMEM((cap, rows, length), jnp.float32),
            pltpu.VMEM(((tiles + 1) * comps, variations, LANES), jnp.float32),
            pltpu.VMEM((variations, 2 * LANES, LANES), jnp.bfloat16),
            pltpu.VMEM((variations, 2 * LANES, LANES), jnp.bfloat16),
            dma((n,)), dma((n,)), dma((n,)), dma((n,)), dma,
            dma((n,)), dma((n,)), dma((n,)), dma((n,)),
        ],
        compiler_params=pltpu.CompilerParams(
            collective_id=0, has_side_effects=True, vmem_limit_bytes=48 << 20),
        name="seismograms",
    )(wants, mechanism, block_count, wants, green_tensors.reshape(held, width, length),
      onset_steps[0], slip_amount[0], slip_rate[0])
    return seismograms[None]


def solution(mesh):
    in_specs = (
        P(("site", "pts"), None, None, None, None),
        P(("site", "pts"), None),
        P(("site", "pts")),
        P(("site", "pts"), None, None),
        P(("site", "pts"), None, None),
        P(("site", "pts"), None),
        P(("site", "pts"), None, None),
    )
    out_specs = P(("site", "pts"), None, None, None)
    return jax.shard_map(local, mesh=mesh, in_specs=in_specs, out_specs=out_specs, check_vma=False)
```

```python
import functools

import jax
import jax.numpy as jnp
from jax import lax
from jax.experimental import pallas as pl
from jax.experimental.pallas import tpu as pltpu
from jax.sharding import PartitionSpec as P

LANES = 128


def seismogram_kernel(n, cap, points, comps, width, listed, wants_s_ref, mech_s_ref, count_ref,
                      wants_ref, green_ref, onset_ref, slip_ref, rate_ref, out_ref,
                      wanted, mech, mechs, wanted_s, outbox, out_scale, inbox, in_scale,
                      motion, high_taps, low_taps, onset_of, slip_of,
                      send_w, recv_w, send_m, recv_m, local_sem, send_t, recv_t, send_s, recv_s):
    me = lax.axis_index("pts")
    rows = points * comps
    length = out_ref.shape[-1]
    tiles = length // LANES
    half = tiles // 2
    strains = width // rows
    variations = onset_ref.shape[0]
    mesh_id = pl.DeviceIdType.MESH
    lane = lax.broadcasted_iota(jnp.int32, (8, LANES), 1)
    sub = lax.broadcasted_iota(jnp.int32, (8, LANES), 0)

    barrier = pltpu.get_barrier_semaphore()

    def greet(d, carry):
        pl.semaphore_signal(barrier, inc=1, device_id={"pts": lax.rem(me + d, n)},
                            device_id_type=mesh_id)
        return carry

    lax.fori_loop(1, n, greet, 0)

    out_row = lax.broadcasted_iota(jnp.int32, (rows, LANES), 0)
    in_row = lax.broadcasted_iota(jnp.int32, (rows, LANES), 1)
    table = jnp.zeros((rows, LANES), jnp.float32)
    for p in range(points):
        for s in range(strains):
            for c in range(comps):
                here = (out_row == p * comps + c) & (in_row == (p * strains + s) * comps + c)
                table = jnp.where(here, mech_s_ref[0, s], table)
    mech[...] = table
    mechs[0] = table
    wanted[0] = wants_ref[me]
    pl.semaphore_wait(barrier, n - 1)

    def remote(src, dst, send, recv, d):
        return pltpu.make_async_remote_copy(
            src_ref=src, dst_ref=dst.at[n - d], send_sem=send.at[d], recv_sem=recv.at[n - d],
            device_id={"pts": lax.rem(me + d, n)}, device_id_type=mesh_id)

    def want_copy(d):
        return remote(wants_ref.at[lax.rem(me + d, n)], wanted, send_w, recv_w, d)

    def mech_copy(d):
        return remote(mech, mechs, send_m, recv_m, d)

    def trace_copy(d):
        return remote(outbox.at[d], inbox, send_t, recv_t, d)

    def scale_copy(d):
        return remote(out_scale.at[d], in_scale, send_s, recv_s, d)

    def start_meta(d, carry):
        want_copy(d).start()
        mech_copy(d).start()
        return carry

    lax.fori_loop(1, n, start_meta, 0)

    i_row = lax.broadcasted_iota(jnp.int32, (LANES, LANES), 0)
    j_lane = lax.broadcasted_iota(jnp.int32, (LANES, LANES), 1)
    near_mask = j_lane >= i_row
    motion[...] = jnp.zeros(motion.shape, jnp.float32)

    for v in range(variations):
        rate = jnp.broadcast_to(rate_ref[v:v + 1, :], (LANES, LANES))
        turned = pltpu.roll(rate, 0, 1, stride=1, stride_axis=0)
        both = jnp.concatenate(
            [jnp.where(near_mask, turned, 0.0), jnp.where(near_mask, 0.0, turned)], axis=0)
        high = both.astype(jnp.bfloat16)
        high_taps[v] = high
        low_taps[v] = (both - high.astype(jnp.float32)).astype(jnp.bfloat16)

    def spread(q, carry):
        pick = jnp.full((variations, LANES), q, jnp.int32)
        onset_of[q] = jnp.take_along_axis(onset_ref[...], pick, axis=1)
        slip_of[q] = jnp.take_along_axis(slip_ref[...], pick, axis=1)
        return carry

    lax.fori_loop(0, listed * points, spread, 0, unroll=4)

    def wait_meta(d, carry):
        want_copy(d).wait()
        mech_copy(d).wait()
        return carry

    lax.fori_loop(1, n, wait_meta, 0)
    to_scalar = pltpu.make_async_copy(wanted, wanted_s, local_sem)
    to_scalar.start()
    to_scalar.wait()

    def encode(d, box, scale_box, at):
        lhs = mechs[d][:, :width]
        high = lhs.astype(jnp.bfloat16).astype(jnp.float32)
        rest = lhs - high
        mid = rest.astype(jnp.bfloat16).astype(jnp.float32)
        stack = jnp.concatenate([high, mid, rest - mid], axis=0).astype(jnp.bfloat16)
        scales = jnp.zeros((8, LANES), jnp.float32)
        for slot in range(cap):
            block = green_ref[wanted_s[d, 0, slot]]
            parts = jnp.dot(stack, block, preferred_element_type=jnp.float32)
            full = parts[0:rows] + (parts[rows:2 * rows] + parts[2 * rows:3 * rows])
            cut = [full[:, i * LANES:(i + 1) * LANES] for i in range(tiles)]
            top = jnp.abs(cut[0])
            for part in cut[1:]:
                top = jnp.maximum(top, jnp.abs(part))
            top = jnp.max(top, axis=1, keepdims=True)
            inverse = 32767.0 / jnp.maximum(top, 1e-30)
            coded = [jnp.floor(part * inverse + 0.5).astype(jnp.int32) for part in cut]
            scales = jnp.where(lane == slot * rows + sub, top * (1.0 / 32767.0), scales)
            for i in range(half):
                word = jnp.bitwise_or(jnp.left_shift(coded[i + half], 16),
                                      jnp.bitwise_and(coded[i], 0xFFFF))
                box[at, slot, :, i * LANES:(i + 1) * LANES] = word
        scale_box[at] = jnp.sum(scales, axis=0, keepdims=True)

    def send(d, carry):
        encode(d, outbox, out_scale, d)

        @pl.when(d > 1)
        def _():
            trace_copy(d - 1).start()
            scale_copy(d - 1).start()

        return carry

    lax.fori_loop(1, n, send, 0)
    encode(0, inbox, in_scale, 0)
    trace_copy(n - 1).start()
    scale_copy(n - 1).start()

    def arrive(step, carry):
        j = lax.rem(n - step, n)
        source_device = lax.rem(me + j, n)

        @pl.when(step > 0)
        def _():
            trace_copy(step).wait_recv()
            scale_copy(step).wait_recv()

        scales = jnp.broadcast_to(in_scale[j], (8, LANES))
        scale_of = [jnp.take_along_axis(scales, jnp.full((8, LANES), q, jnp.int32), axis=1)
                    for q in range(cap * rows)]
        for group in range(variations // 8):
            acc = [motion[comps + q, group * 8:group * 8 + 8, :] for q in range(tiles * comps)]
            for slot in range(cap):
                k = wants_s_ref[source_device, 0, cap + slot]
                used = jnp.where(jnp.full((8, LANES), k, jnp.int32) < count_ref[0], 1.0, 0.0)
                base = jnp.minimum(k, listed - 1) * points
                for p in range(points):
                    onset = onset_of[base + p, group * 8:group * 8 + 8, :]
                    slip = slip_of[base + p, group * 8:group * 8 + 8, :] * used
                    shift = jnp.bitwise_and(onset, LANES - 1)
                    back = jnp.right_shift(onset, 7) + (lane >= LANES - shift).astype(jnp.int32)
                    one = back >= 1
                    two = back >= 2
                    source = jnp.bitwise_and(lane - shift, LANES - 1)
                    for c in range(comps):
                        row = p * comps + c
                        weight = slip * scale_of[slot * rows + row]
                        words = [jnp.broadcast_to(
                            inbox[j, slot, row:row + 1, i * LANES:(i + 1) * LANES], (8, LANES))
                            for i in range(half)]
                        prev2 = jnp.left_shift(words[half - 2], 16)
                        prev1 = jnp.left_shift(words[half - 1], 16)
                        for i in range(half):
                            cur = words[i]
                            mixed = jnp.where(two, prev2, jnp.where(one, prev1, cur))
                            moved = jnp.take_along_axis(mixed, source, axis=1)
                            low = jnp.right_shift(jnp.left_shift(moved, 16), 16)
                            high = jnp.right_shift(moved, 16)
                            acc[i * comps + c] += weight * low.astype(jnp.float32)
                            acc[(i + half) * comps + c] += weight * high.astype(jnp.float32)
                            prev2, prev1 = prev1, cur
            for q in range(tiles * comps):
                motion[comps + q, group * 8:group * 8 + 8, :] = acc[q]
        return carry

    lax.fori_loop(0, n, arrive, 0)

    count = tiles * comps
    for v in range(variations):
        lhs = jnp.concatenate([motion[comps:comps + count, v, :], motion[0:count, v, :]], axis=1)
        high = lhs.astype(jnp.bfloat16).astype(jnp.float32)
        pair = jnp.concatenate([high, lhs - high], axis=0).astype(jnp.bfloat16)
        main = jnp.dot(pair, high_taps[v], preferred_element_type=jnp.float32)
        minor = jnp.dot(pair[:count], low_taps[v], preferred_element_type=jnp.float32)
        result = main[:count] + (main[count:] + minor)
        for i in range(tiles):
            out_ref[v, :, i * LANES:(i + 1) * LANES] = result[i * comps:(i + 1) * comps, :]

    def wait_sent(d, carry):
        trace_copy(d).wait_send()
        scale_copy(d).wait_send()
        return carry

    lax.fori_loop(1, n, wait_sent, 0)


def local(green_tensors, block_lists, block_count, onset_steps, slip_amount, mechanism, slip_rate):
    held, points, strains, comps, length = green_tensors.shape
    ruptures, listed = block_lists.shape
    assert ruptures == 1
    variations = onset_steps.shape[1]
    n = lax.axis_size("pts")
    cap = max(1, listed // n)
    width = points * strains * comps
    rows = points * comps
    tiles = length // LANES
    assert cap * rows <= LANES

    blocks = block_lists.reshape(listed)
    holder = blocks // held
    order = jnp.arange(listed, dtype=jnp.int32)
    rank = jnp.sum(((holder[:, None] == holder[None, :]) & (order[None, :] < order[:, None]))
                   .astype(jnp.int32), axis=1)
    lanes = jnp.arange(LANES, dtype=jnp.int32)
    hit = (holder[None, None, :] == jnp.arange(n, dtype=jnp.int32)[:, None, None]) & (
        rank[None, None, :] == (lanes % cap)[None, :, None])
    value = jnp.where((lanes < cap)[None, :, None], (blocks % held)[None, None, :],
                      (order - listed)[None, None, :])
    wants = jnp.sum(jnp.where(hit, value, 0), axis=2) + jnp.where(lanes < cap, 0, listed)[None, :]
    wants = wants.astype(jnp.int32).reshape(n, 1, LANES)

    vmem = pl.BlockSpec(memory_space=pltpu.VMEM)
    smem = pl.BlockSpec(memory_space=pltpu.SMEM)
    dma = pltpu.SemaphoreType.DMA
    seismograms = pl.pallas_call(
        functools.partial(seismogram_kernel, n, cap, points, comps, width, listed),
        out_shape=jax.ShapeDtypeStruct((variations, comps, length), jnp.float32),
        in_specs=[smem, smem, smem, vmem, vmem, vmem, vmem, vmem],
        out_specs=vmem,
        scratch_shapes=[
            pltpu.VMEM((n, 1, LANES), jnp.int32),
            pltpu.VMEM((rows, LANES), jnp.float32),
            pltpu.VMEM((n, rows, LANES), jnp.float32),
            pltpu.SMEM((n, 1, LANES), jnp.int32),
            pltpu.VMEM((n, cap, rows, length // 2), jnp.int32),
            pltpu.VMEM((n, 1, LANES), jnp.float32),
            pltpu.VMEM((n, cap, rows, length // 2), jnp.int32),
            pltpu.VMEM((n, 1, LANES), jnp.float32),
            pltpu.VMEM(((tiles + 1) * comps, variations, LANES), jnp.float32),
            pltpu.VMEM((variations, 2 * LANES, LANES), jnp.bfloat16),
            pltpu.VMEM((variations, 2 * LANES, LANES), jnp.bfloat16),
            pltpu.VMEM((listed * points, variations, LANES), jnp.int32),
            pltpu.VMEM((listed * points, variations, LANES), jnp.float32),
            dma((n,)), dma((n,)), dma((n,)), dma((n,)), dma,
            dma((n,)), dma((n,)), dma((n,)), dma((n,)),
        ],
        compiler_params=pltpu.CompilerParams(
            collective_id=0, has_side_effects=True, vmem_limit_bytes=48 << 20),
        name="seismograms",
    )(wants, mechanism, block_count, wants, green_tensors.reshape(held, width, length),
      onset_steps[0], slip_amount[0], slip_rate[0])
    return seismograms[None]


def solution(mesh):
    in_specs = (
        P(("site", "pts"), None, None, None, None),
        P(("site", "pts"), None),
        P(("site", "pts")),
        P(("site", "pts"), None, None),
        P(("site", "pts"), None, None),
        P(("site", "pts"), None),
        P(("site", "pts"), None, None),
    )
    out_specs = P(("site", "pts"), None, None, None)
    return jax.shard_map(local, mesh=mesh, in_specs=in_specs, out_specs=out_specs, check_vma=False)
```
